32 devices in a mesh: rep: 4 (over y, core), ep: 4 (over z), tp: 2 (over x).
Axes of the slice: x: 2, y: 2, z: 4, core: 2. Of those that a mesh axis runs over, the one named last changes fastest.
Arguments:
- tokens: bfloat16 [128, 6144], P(('rep', 'ep'), 'tp'), may hold values from -6 to 6
- expert_ids: int32 [128, 2], P(('rep', 'ep')), may hold values from 0 to 3, as said below
- replicas: int32 [128, 2], P(('rep', 'ep')), may hold values from 0 to 3, as said below
- scores: float32 [128, 2], P(('rep', 'ep')), may hold values from -8 to 8
- w_gate: bfloat16 [4, 6144, 1024], P('ep', None, 'tp'), may hold values from -0.078125 to 0.078125
- w_up: bfloat16 [4, 6144, 1024], P('ep', None, 'tp'), may hold values from -0.078125 to 0.078125
- w_down: bfloat16 [4, 1024, 6144], P('ep', 'tp'), may hold values from -0.1875 to 0.1875
Outputs:
- moe_out: bfloat16 [128, 6144], P(('rep', 'ep'), 'tp')
- load_counts: int32 [4, 4], replicated
The draws below stay inside these ranges and needn't reach their ends.
Inputs may be any that keep to these rules, and one draw needn't show every extreme that they name: `expert_ids`: each row names 2 different experts. In the rows of one device one expert is named by every row. `replicas`: in the rows of one device at most 2 pairs name the same expert with the same replica pick, and some expert and pick reach 2.
All inputs are finite; a program needn't handle non-finite values.
Results may differ from the reference program's by a relative error of at most 0.008.
Values may be sent and summed in bfloat16 or wider, within the bound.
A program may use at most 64 MiB of HBM per device.

```python
import jax
import jax.numpy as jnp
from jax import lax

D = 6144
FFE = 1024
TOK_DEV = 8
REPL = 4
EXPERTS = 4
TOPK = 2
TOKENS = 128
N_REP = 4
N_EP = 4


def routing_tables(key):
    blocks = TOKENS // TOK_DEV
    key_hot = jax.random.fold_in(key, 101)
    key_rest = jax.random.fold_in(key, 102)
    key_roll = jax.random.fold_in(key, 103)
    key_offset = jax.random.fold_in(key, 104)
    hot_block = jax.random.randint(key_hot, (blocks,), 0, EXPERTS).astype(jnp.int32)
    hot_token = jnp.repeat(hot_block, TOK_DEV)
    raw_bits = jax.random.randint(key_rest, (TOKENS, EXPERTS), 0, 1 << 20).astype(jnp.int32)
    column_ids = jnp.arange(EXPERTS, dtype=jnp.int32)
    ranked = raw_bits * EXPERTS + column_ids[None, :]
    ranked = jnp.where(column_ids[None, :] == hot_token[:, None], -1, ranked)
    unused, others = lax.top_k(ranked, TOPK - 1)
    chosen = jnp.concatenate([hot_token[:, None], others.astype(jnp.int32)], 1)
    rolled = jax.random.randint(key_roll, (TOKENS, 1), 0, TOPK).astype(jnp.int32)
    position = (jnp.arange(TOPK, dtype=jnp.int32)[None, :] + rolled) % TOPK
    chosen = jnp.take_along_axis(chosen, position, 1)
    named = jnp.sum((chosen[:, :, None] == column_ids[None, None, :]).astype(jnp.int32), 1)
    named_blocks = named.reshape(blocks, TOK_DEV, EXPERTS)
    earlier = (jnp.cumsum(named_blocks, 1) - named_blocks).reshape(TOKENS, EXPERTS)
    offsets = jax.random.randint(key_offset, (blocks, EXPERTS), 0, REPL).astype(jnp.int32)
    offset_token = jnp.repeat(offsets, TOK_DEV, axis=0)
    copy_table = (earlier + offset_token) % REPL
    copies = jnp.take_along_axis(copy_table, chosen, 1)
    return (chosen.astype(jnp.int32), copies.astype(jnp.int32))


def draw_expert_ids(key, part):
    chosen, copies = routing_tables(key)
    return chosen


def draw_replicas(key, part):
    chosen, copies = routing_tables(key)
    return copies


def block_scale(rng, extent, split, smallest, largest):
    loudness = 1.0
    for dim, parts in split:
        draws = jax.random.uniform(jax.random.fold_in(jax.random.fold_in(rng, 6), dim), (parts,), jnp.float32, smallest / len(split), largest / len(split))
        loudness = loudness * jnp.repeat(jnp.exp(draws), extent[dim] // parts).reshape((-1,) + (1,) * (len(extent) - 1 - dim))
    return loudness


def scatter_about(own_key, extent, deviation, most, shards=(), held_as=jnp.bfloat16):
    factor_of = block_scale(own_key, extent, shards, -0.22, 0.18) if shards else 1.0
    entries = jax.random.normal(own_key, extent, jnp.float32) * deviation * factor_of
    return jnp.minimum(jnp.maximum(entries, -most), most).astype(held_as)


def setup_inputs(seed: int = 0) -> dict:
    key_list = jax.random.split(jax.random.key(seed), 8)
    tokens = scatter_about(key_list[0], (TOKENS, D), 1.0, 6.0, ((0, 16), (1, 2)))
    expert_ids = draw_expert_ids(jax.random.fold_in(key_list[7], 71), 0)
    replicas = draw_replicas(jax.random.fold_in(key_list[7], 71), 0)
    scores = scatter_about(key_list[3], (TOKENS, TOPK), 2.0, 8.0, ((0, 16),), jnp.float32)
    w_gate = scatter_about(key_list[4], (EXPERTS, D, FFE), D ** -0.5, 0.078125, ((0, 4), (2, 2)))
    w_up = scatter_about(key_list[5], (EXPERTS, D, FFE), D ** -0.5, 0.078125, ((0, 4), (2, 2)))
    w_down = scatter_about(key_list[6], (EXPERTS, FFE, D), FFE ** -0.5, 0.1875, ((0, 4), (1, 2)))
    return {"tokens": tokens, "expert_ids": expert_ids, "replicas": replicas, "scores": scores, "w_gate": w_gate, "w_up": w_up, "w_down": w_down}


route_scale = 2.5


def reference(tokens, expert_ids, replicas, scores, w_gate, w_up, w_down):
    sigmoid_scores = jax.nn.sigmoid(scores)
    weights = sigmoid_scores / jnp.sum(sigmoid_scores, 1, keepdims=True) * route_scale

    def serve(running, expert):
        matched = expert_ids == expert
        coefficient = jnp.sum(jnp.where(matched, weights, jnp.zeros_like(weights)), 1)
        gate_pre = jnp.dot(tokens, w_gate[expert], preferred_element_type=jnp.float32)
        up_pre = jnp.dot(tokens, w_up[expert], preferred_element_type=jnp.float32)
        hidden = (jax.nn.silu(gate_pre) * up_pre).astype(jnp.bfloat16)
        expert_out = jnp.dot(hidden, w_down[expert], preferred_element_type=jnp.float32).astype(jnp.bfloat16)
        return running + coefficient[:, None] * expert_out.astype(jnp.float32), None

    start_total = jnp.zeros((TOKENS, D), jnp.float32)
    running, unused = lax.scan(serve, start_total, jnp.arange(EXPERTS, dtype=jnp.int32))
    moe_out = running.astype(jnp.bfloat16)
    source_group = (jnp.arange(TOKENS, dtype=jnp.int32) // (TOK_DEV * N_EP))[:, None]
    target = (source_group + replicas * (N_REP // REPL)) % N_REP
    group_hit = target.reshape(-1)[:, None, None] == jnp.arange(N_REP, dtype=jnp.int32)[None, :, None]
    expert_hit = expert_ids.reshape(-1)[:, None, None] == jnp.arange(EXPERTS, dtype=jnp.int32)[None, None, :]
    load_counts = jnp.sum((group_hit & expert_hit).astype(jnp.int32), 0)
    return moe_out, load_counts
```

```python
import functools

import jax
import jax.numpy as jnp
from jax import lax
from jax.experimental import pallas as pl
from jax.experimental.pallas import tpu as pltpu
from jax.sharding import PartitionSpec as P

REPL = 4
route_scale = 2.5
GATHER_CHUNKS = 3
RETURN_CHUNKS = 4
MESH = pl.DeviceIdType.MESH


def stable_sigmoid(v):
    small = jnp.exp(-jnp.abs(v))
    return jnp.where(v >= 0, 1.0, small) / (1.0 + small)


def kernel(
    sizes,
    tokens_hbm, ids_hbm, replicas_hbm, scores_hbm, gate_hbm, up_hbm, down_hbm,
    out_ref, counts_ref,
    ids_ref, replicas_ref, scores_ref,
    x_buf, gate_buf, up_buf, down_buf,
    own_sum, tp_send, tp_recv, ep_send, ep_recv,
    count_own, count_ep, count_mid, count_rep,
    token_sem, table_sem, weight_sem,
    gather_recv, gather_ep_send, gather_tp_send,
    tp_send_sem, tp_recv_sem, ep_send_sem, ep_recv_sem,
    count_ep_send, count_ep_recv, count_rep_send, count_rep_recv,
):
    reps, eps, tps, rows, width = sizes
    stride = reps // REPL
    me_rep, me_ep, me_tp = lax.axis_index("rep"), lax.axis_index("ep"), lax.axis_index("tp")
    rep_peer = lambda o: {"rep": lax.rem(me_rep + o, reps)}
    ep_peer = lambda o: {"ep": lax.rem(me_ep + o, eps)}
    tp_peer = lambda o: {"tp": lax.rem(me_tp + o, tps)}
    g_chunk = width // GATHER_CHUNKS
    r_chunk = width // RETURN_CHUNKS
    top_k = ids_ref.shape[0]

    def remote(src, dst, send, recv, device):
        return pltpu.make_async_remote_copy(
            src_ref=src, dst_ref=dst, send_sem=send, recv_sem=recv,
            device_id=device, device_id_type=MESH,
        )

    barrier = pltpu.get_barrier_semaphore()
    peers = (
        [ep_peer(o) for o in range(1, eps)]
        + [tp_peer(o) for o in range(1, tps)]
        + [rep_peer(o) for o in range(1, reps)]
    )
    for peer in peers:
        pl.semaphore_signal(barrier, inc=1, device_id=peer, device_id_type=MESH)

    token_copies = []
    for c in range(GATHER_CHUNKS):
        copy = pltpu.make_async_copy(
            tokens_hbm.at[:, pl.ds(c * g_chunk, g_chunk)], x_buf.at[0, c, 0], token_sem.at[c]
        )
        copy.start()
        token_copies.append(copy)
    table_copies = []
    for k, (src, dst) in enumerate(((ids_hbm, ids_ref), (replicas_hbm, replicas_ref), (scores_hbm, scores_ref))):
        copy = pltpu.make_async_copy(src, dst, table_sem.at[k])
        copy.start()
        table_copies.append(copy)

    for copy in token_copies + table_copies:
        copy.wait()
    weight_copies = {}
    for d in range(tps):
        start = pl.multiple_of(lax.rem(me_tp + d, tps) * width, width)
        for k, (src, dst) in enumerate(((gate_hbm, gate_buf), (up_hbm, up_buf))):
            copy = pltpu.make_async_copy(src.at[0, pl.ds(start, width), :], dst.at[d], weight_sem.at[k, d])
            copy.start()
            weight_copies[k, d] = copy
    for d in list(range(1, tps)) + [0]:
        start = pl.multiple_of(lax.rem(me_tp + d, tps) * width, width)
        copy = pltpu.make_async_copy(down_hbm.at[0, :, pl.ds(start, width)], down_buf.at[d], weight_sem.at[2, d])
        copy.start()
        weight_copies[2, d] = copy

    diagonal = lax.broadcasted_iota(jnp.int32, (rows, rows), 0) == lax.broadcasted_iota(jnp.int32, (rows, rows), 1)

    def columns(ref):
        table = ref[...]
        zero = jnp.zeros((), table.dtype)
        return [
            jnp.sum(jnp.where(diagonal, table[k : k + 1, :], zero), 1, keepdims=True)
            for k in range(top_k)
        ]

    ids = columns(ids_ref)
    target = [lax.rem(me_rep + r * stride, reps) for r in columns(replicas_ref)]
    expert_lane = lax.broadcasted_iota(jnp.int32, (rows, count_own.shape[1]), 1)
    count_own[...] = jnp.zeros_like(count_own)
    hits = [ids[k] == expert_lane for k in range(top_k)]
    for g in range(reps):
        total = jnp.zeros(expert_lane.shape, jnp.float32)
        for k in range(top_k):
            total += jnp.where(hits[k] & (target[k] == g), 1.0, 0.0)
        count_own[g : g + 1, :] = jnp.sum(total, 0, keepdims=True).astype(jnp.int32)

    sigmoid_scores = [stable_sigmoid(v) for v in columns(scores_ref)]
    norm = sum(sigmoid_scores)
    weights = [v / norm * route_scale for v in sigmoid_scores]
    coefficients = []
    for s in range(eps):
        expert = lax.rem(me_ep + s, eps)
        coefficients.append(sum(jnp.where(ids[k] == expert, weights[k], 0.0) for k in range(top_k)))

    pl.semaphore_wait(barrier, len(peers))
    pending = []

    for c in range(GATHER_CHUNKS):
        for o in range(eps - 1, 0, -1):
            copy = remote(
                x_buf.at[0, c, 0], x_buf.at[0, c, eps - o],
                gather_ep_send.at[c, o], gather_recv.at[0, c, eps - o], ep_peer(o),
            )
            copy.start()
            pending.append(copy)
        for d in range(1, tps):
            copy = remote(
                x_buf.at[0, c, 0], x_buf.at[tps - d, c, 0],
                gather_tp_send.at[d, c, 0], gather_recv.at[tps - d, c, 0], tp_peer(d),
            )
            copy.start()
            pending.append(copy)

    def gather_wait(d, c, s):
        pltpu.make_async_copy(x_buf.at[d, c, s], x_buf.at[d, c, s], gather_recv.at[d, c, s]).wait()

    count_copies = []
    for o in range(1, eps):
        copy = remote(count_own, count_ep.at[o], count_ep_send.at[o], count_ep_recv.at[o], ep_peer(o))
        copy.start()
        count_copies.append(copy)

    for c in range(GATHER_CHUNKS):
        for o in range(eps - 1, 0, -1):
            s = eps - o
            gather_wait(0, c, s)
            for d in range(1, tps):
                copy = remote(
                    x_buf.at[0, c, s], x_buf.at[tps - d, c, s],
                    gather_tp_send.at[d, c, s], gather_recv.at[tps - d, c, s], tp_peer(d),
                )
                copy.start()
                pending.append(copy)

    hidden_count = gate_buf.shape[2]
    gate = jnp.zeros((eps * rows, hidden_count), jnp.float32)
    up = jnp.zeros((eps * rows, hidden_count), jnp.float32)
    for d in range(tps):
        for k in range(2):
            weight_copies[k, d].wait()
        for c in range(GATHER_CHUNKS):
            if d > 0:
                for s in range(eps):
                    gather_wait(d, c, s)
            x = x_buf[d, c].astype(jnp.float32).reshape(eps * rows, g_chunk).astype(jnp.bfloat16)
            gate += jnp.dot(x, gate_buf[d, pl.ds(c * g_chunk, g_chunk), :], preferred_element_type=jnp.float32)
            up += jnp.dot(x, up_buf[d, pl.ds(c * g_chunk, g_chunk), :], preferred_element_type=jnp.float32)
    hidden = (gate * stable_sigmoid(gate) * up).astype(jnp.bfloat16)

    mid = count_own[...]
    for o in range(1, eps):
        count_copies[o - 1].wait_recv()
        mid += count_ep[o]
    count_mid[...] = mid
    rep_copies = []
    for o in range(1, reps):
        copy = remote(count_mid, count_rep.at[o], count_rep_send.at[o], count_rep_recv.at[o], rep_peer(o))
        copy.start()
        rep_copies.append(copy)

    tp_copies = {}
    for d in list(range(1, tps)) + [0]:
        weight_copies[2, d].wait()
        for c in range(RETURN_CHUNKS):
            part = jnp.dot(hidden, down_buf[d, :, pl.ds(c * r_chunk, r_chunk)], preferred_element_type=jnp.float32)
            part = part.reshape(eps, rows, r_chunk)
            if d == 0:
                own_sum[c] = part
                continue
            tp_send[d - 1, c] = part.astype(jnp.bfloat16)
            copy = remote(
                tp_send.at[d - 1, c], tp_recv.at[d - 1, c],
                tp_send_sem.at[d - 1, c], tp_recv_sem.at[d - 1, c], tp_peer(d),
            )
            copy.start()
            tp_copies[d, c] = copy

    ep_copies = {}
    for c in range(RETURN_CHUNKS):
        total = own_sum[c]
        for d in range(1, tps):
            tp_copies[d, c].wait_recv()
            total += tp_recv[d - 1, c].astype(jnp.float32)
        ep_send[c] = total.astype(jnp.bfloat16)
        for o in range(1, eps):
            copy = remote(
                ep_send.at[c, o], ep_recv.at[c, eps - o],
                ep_send_sem.at[c, o], ep_recv_sem.at[c, eps - o], ep_peer(o),
            )
            copy.start()
            ep_copies[c, o] = copy

    final = count_mid[...]
    for o in range(1, reps):
        rep_copies[o - 1].wait_recv()
        final += count_rep[o]
    counts_ref[...] = final[:reps, :eps]

    for c in range(RETURN_CHUNKS):
        total = coefficients[0] * ep_send[c, 0].astype(jnp.float32)
        for s in range(1, eps):
            pltpu.make_async_copy(ep_recv.at[c, s], ep_recv.at[c, s], ep_recv_sem.at[c, s]).wait()
            total += coefficients[s] * ep_recv[c, s].astype(jnp.float32)
        out_ref[:, pl.ds(c * r_chunk, r_chunk)] = total.astype(out_ref.dtype)

    for copy in pending + count_copies + rep_copies + list(tp_copies.values()) + list(ep_copies.values()):
        copy.wait_send()


def per_device(tokens, expert_ids, replicas, scores, w_gate, w_up, w_down):
    reps, eps, tps = lax.axis_size("rep"), lax.axis_size("ep"), lax.axis_size("tp")
    rows, width = tokens.shape
    hidden = w_gate.shape[2]
    g_chunk, r_chunk = width // GATHER_CHUNKS, width // RETURN_CHUNKS
    sizes = (reps, eps, tps, rows, width)
    vmem = pl.BlockSpec(memory_space=pltpu.VMEM)
    hbm = pl.BlockSpec(memory_space=pl.ANY)
    lanes = 128
    count_rows = -(-reps // 8) * 8
    dma = pltpu.SemaphoreType.DMA
    bf16, f32, i32 = jnp.bfloat16, jnp.float32, jnp.int32
    moe, counts = pl.pallas_call(
        functools.partial(kernel, sizes),
        out_shape=(
            pltpu.VMEM((rows, width), bf16),
            pltpu.VMEM((reps, eps), i32),
        ),
        in_specs=[hbm] * 7,
        out_specs=(vmem, vmem),
        scratch_shapes=[
            pltpu.VMEM(expert_ids.shape[::-1], i32),
            pltpu.VMEM(replicas.shape[::-1], i32),
            pltpu.VMEM(scores.shape[::-1], f32),
            pltpu.VMEM((tps, GATHER_CHUNKS, eps, rows, g_chunk), bf16),
            pltpu.VMEM((tps, width, hidden), bf16),
            pltpu.VMEM((tps, width, hidden), bf16),
            pltpu.VMEM((tps, hidden, width), bf16),
            pltpu.VMEM((RETURN_CHUNKS, eps, rows, r_chunk), f32),
            pltpu.VMEM((tps - 1, RETURN_CHUNKS, eps, rows, r_chunk), bf16),
            pltpu.VMEM((tps - 1, RETURN_CHUNKS, eps, rows, r_chunk), bf16),
            pltpu.VMEM((RETURN_CHUNKS, eps, rows, r_chunk), bf16),
            pltpu.VMEM((RETURN_CHUNKS, eps, rows, r_chunk), bf16),
            pltpu.VMEM((count_rows, lanes), i32),
            pltpu.VMEM((eps, count_rows, lanes), i32),
            pltpu.VMEM((count_rows, lanes), i32),
            pltpu.VMEM((reps, count_rows, lanes), i32),
            dma((GATHER_CHUNKS,)),
            dma((3,)),
            dma((3, tps)),
            dma((tps, GATHER_CHUNKS, eps)),
            dma((GATHER_CHUNKS, eps)),
            dma((tps, GATHER_CHUNKS, eps)),
            dma((tps - 1, RETURN_CHUNKS)),
            dma((tps - 1, RETURN_CHUNKS)),
            dma((RETURN_CHUNKS, eps)),
            dma((RETURN_CHUNKS, eps)),
            dma((eps,)),
            dma((eps,)),
            dma((reps,)),
            dma((reps,)),
        ],
        compiler_params=pltpu.CompilerParams(
            collective_id=0, has_side_effects=True, vmem_limit_bytes=56 * 1024 * 1024
        ),
    )(tokens, expert_ids.T, replicas.T, scores.T, w_gate, w_up, w_down)
    return pl.pallas_call(
        finish,
        out_shape=(jax.ShapeDtypeStruct(moe.shape, moe.dtype), jax.ShapeDtypeStruct(counts.shape, counts.dtype)),
        in_specs=[vmem, vmem],
        out_specs=(hbm, hbm),
        scratch_shapes=[dma((2,))],
    )(pltpu.with_memory_space_constraint(moe, pltpu.VMEM), pltpu.with_memory_space_constraint(counts, pltpu.VMEM))


def finish(moe_ref, counts_ref, moe_out, counts_out, sem):
    a = pltpu.make_async_copy(moe_ref, moe_out, sem.at[0])
    b = pltpu.make_async_copy(counts_ref, counts_out, sem.at[1])
    a.start()
    b.start()
    a.wait()
    b.wait()


def solution(mesh):
    placed = (
        P(("rep", "ep"), "tp"),
        P(("rep", "ep"), None),
        P(("rep", "ep"), None),
        P(("rep", "ep"), None),
        P("ep", None, "tp"),
        P("ep", None, "tp"),
        P("ep", "tp", None),
    )
    return jax.shard_map(
        per_device,
        mesh=mesh,
        in_specs=placed,
        out_specs=(P(("rep", "ep"), "tp"), P()),
        check_vma=False,
    )
```
